32 devices in a mesh: seq: 16 (over z, x, core), head: 2 (over y).
Axes of the slice: x: 2, y: 2, z: 4, core: 2. Of those that a mesh axis runs over, the one named last changes fastest.
Arguments:
- query_rows: bfloat16 [3072, 2048], P('seq', 'head'), may hold values from -6 to 6
- key_rows: bfloat16 [3072, 2048], P('seq', 'head'), may hold values from -6 to 6
- value_rows: bfloat16 [3072, 2048], P('seq', 'head'), may hold values from -6 to 6
- grad_output: bfloat16 [3072, 2048], P('seq', 'head'), may hold values from -6 to 6
- positions: int32 [3072], P('seq'), may hold values from 0 to 3071, each once
Outputs:
- grad_query: bfloat16 [3072, 2048], P(('seq', 'head'))
- grad_keys: bfloat16 [3072, 2048], P('seq', 'head')
- grad_values: bfloat16 [3072, 2048], P('seq', 'head')
The draws below stay inside these ranges and needn't reach their ends.
Inputs may be any that keep to these rules, and one draw needn't show every extreme that they name: `positions`: each number from 0 to 3071 appears once.
All inputs are finite; a program needn't handle non-finite values.
Results may differ from the reference program's by a relative error of at most 0.012.
Values may be sent and summed in bfloat16 or wider, within the bound.
A program may use at most 128 MiB of HBM per device.

```python
import jax
import jax.numpy as jnp
from jax import lax

HEADS = 16
HEAD_DIM = 128
TOKENS = 3072


def base_rows(key, salt):
    noise_key = jax.random.fold_in(jax.random.fold_in(key, salt), 0)
    drawn = jax.random.normal(noise_key, (TOKENS, HEADS * HEAD_DIM), jnp.float32)
    return jnp.clip(drawn, -6.0, 6.0)


def draw_query_rows(key, part):
    drawn = base_rows(key, 1)
    return drawn.astype(jnp.bfloat16)


def draw_key_rows(key, part):
    drawn = base_rows(key, 2)
    return drawn.astype(jnp.bfloat16)


def block_levels(rng, shape, shards, smallest, high):
    def one(position, parts):
        heights = jax.random.uniform(jax.random.fold_in(jax.random.fold_in(rng, 6), position), (parts,), jnp.float32, smallest / len(shards), high / len(shards))
        return jnp.repeat(jnp.exp(heights), shape[position] // parts).reshape((-1,) + (1,) * (len(shape) - position - 1))

    factor_of = one(*shards[0])
    for cut in shards[1:]:
        factor_of = factor_of * one(*cut)
    return factor_of


def scatter_about(rng, extent, spread, most, cuts=(), held_as=jnp.bfloat16):
    entries = jax.random.normal(rng, extent, jnp.float32) * spread
    if len(cuts) > 0:
        entries = block_levels(rng, extent, cuts, -0.22, 0.18) * entries
    return jnp.clip(entries, min=-most, max=most).astype(held_as)


def setup_inputs(seed: int = 0) -> dict:
    streams_of = jax.random.split(jax.random.key(seed), 6)
    return {
        "query_rows": draw_query_rows(jax.random.fold_in(streams_of[5], 71), 0),
        "key_rows": draw_key_rows(jax.random.fold_in(streams_of[5], 71), 0),
        "value_rows": scatter_about(streams_of[2], (TOKENS, HEADS * HEAD_DIM), 1.0, 6.0, ((0, 16), (1, 2))),
        "grad_output": scatter_about(streams_of[3], (TOKENS, HEADS * HEAD_DIM), 1.0, 6.0, ((0, 16), (1, 2))),
        "positions": jax.random.permutation(streams_of[4], TOKENS).astype(jnp.int32),
    }


def reference(query_rows, key_rows, value_rows, grad_output, positions):
    tokens = query_rows.shape[0]
    scaling = HEAD_DIM ** -0.5
    allowed = positions[None, :] <= positions[:, None]

    def per_head(matrix):
        return jnp.swapaxes(matrix.reshape(tokens, HEADS, HEAD_DIM), 0, 1)

    def back_rows(matrix):
        return jnp.swapaxes(matrix, 0, 1).reshape(tokens, HEADS * HEAD_DIM)

    def one_head(head_items):
        query_full = head_items[0].astype(jnp.float32)
        key_full = head_items[1].astype(jnp.float32)
        value_full = head_items[2].astype(jnp.float32)
        grad_full = head_items[3].astype(jnp.float32)
        highest = lax.Precision.HIGHEST
        scores = jnp.dot(query_full, key_full.T, precision=highest) * scaling
        masked = jnp.where(allowed, scores, -1.0e30)
        top_score = jnp.max(masked, axis=1)
        denominator = jnp.sum(jnp.where(allowed, jnp.exp(masked - top_score[:, None]), 0.0), axis=1)
        log_total = top_score + jnp.log(denominator)
        probabilities = jnp.where(allowed, jnp.exp(masked - log_total[:, None]), 0.0)
        weights = probabilities.astype(jnp.bfloat16).astype(jnp.float32)
        grad_probs = jnp.dot(grad_full, value_full.T, precision=highest)
        row_delta = jnp.sum(probabilities * grad_probs, axis=1)
        grad_value = jnp.dot(weights.T, grad_full, precision=highest)
        grad_scores = (probabilities * (grad_probs - row_delta[:, None]) * scaling).astype(jnp.bfloat16).astype(jnp.float32)
        grad_query = jnp.dot(grad_scores, key_full, precision=highest)
        grad_key = jnp.dot(grad_scores.T, query_full, precision=highest)
        return grad_query.astype(jnp.bfloat16), grad_key.astype(jnp.bfloat16), grad_value.astype(jnp.bfloat16)

    grad_query, grad_keys, grad_values = lax.map(one_head, (per_head(query_rows), per_head(key_rows), per_head(value_rows), per_head(grad_output)))
    return back_rows(grad_query), back_rows(grad_keys), back_rows(grad_values)
```

```python
import functools
import math

import jax
import jax.numpy as jnp
from jax import lax
from jax.experimental import pallas as pl
from jax.experimental.pallas import tpu as pltpu
from jax.sharding import PartitionSpec as P

HEAD_DIM = 128
MESH = pl.DeviceIdType.MESH
NT = (((1,), (1,)), ((), ()))
LOW = -1e30


def kernel(
    members, heads, groups, rows, width, pair, step,
    pos_ref, q_hbm, k_hbm, v_hbm, g_hbm,
    dq_out, dk_out, dv_out,
    qg_buf, kv_buf, qg_stage, kv_stage, key_t, pos_mine, pos_buf, key_pos, tops,
    z_buf, p_buf, dk_acc, dv_acc, stat_buf, kv_final, kv_back, dq_stage, dq_back,
    qg_local, kv_local, qg_send, qg_recv, kv_send, kv_recv, pos_send, pos_recv,
    stat_send, stat_recv, back_send, back_recv, dq_send, dq_recv,
):
    ratio = members // heads
    units = members // pair
    wide = heads // pair
    me = lax.axis_index("seq")
    group = lax.axis_index("head")
    mine = lax.rem(me, heads)
    mates = me // heads
    place = mine // pair
    core = lax.rem(mine, pair)
    scaling = HEAD_DIM ** (-0.5)
    sharp = scaling / math.log(2.0)
    block = pair * rows
    keys = heads * rows
    steps = heads // step
    part_rows = rows // groups

    def columns(index):
        return pl.ds(pl.multiple_of(index * HEAD_DIM, HEAD_DIM), HEAD_DIM)

    kv_order = [lax.rem(mine + j, heads) for j in range(heads)]

    def target(t, c):
        return lax.rem(place + wide - t, wide) * pair + lax.rem(core + c, pair)

    near = [(t, c) for t in range(wide) for c in range(pair)]

    def local_copies(arrays, index, first, stage, sems, j):
        return [
            pltpu.make_async_copy(
                array.at[:, columns(index)], first.at[a] if j == 0 else stage.at[j, a],
                sems.at[a, j],
            )
            for a, array in enumerate(arrays)
        ]

    kv_locals = [
        local_copies((k_hbm, v_hbm), kv_order[j], kv_buf.at[mine], kv_stage, kv_local, j)
        for j in range(heads)
    ]
    qg_locals = [
        local_copies((q_hbm, g_hbm), target(t, c), qg_buf.at[me], qg_stage, qg_local, j)
        for j, (t, c) in enumerate(near)
    ]
    for copies in kv_locals[1:] + qg_locals + kv_locals[:1]:
        for copy in copies:
            copy.start()

    pos_mine[...] = pos_ref[...]
    barrier = pltpu.get_barrier_semaphore()
    for d in range(members):
        for e in range(groups):
            if d or e:
                pl.semaphore_signal(
                    barrier, inc=1,
                    device_id={
                        "seq": lax.rem(me + d, members), "head": lax.rem(group + e, groups),
                    },
                    device_id_type=MESH,
                )
    pl.semaphore_wait(barrier, members * groups - 1)

    def remote(source, sink, send, recv, seq, head):
        return pltpu.make_async_remote_copy(
            src_ref=source, dst_ref=sink, send_sem=send, recv_sem=recv,
            device_id={"seq": seq, "head": head}, device_id_type=MESH,
        )

    def pos_copy(d, origin):
        return remote(
            pos_mine, pos_buf.at[origin], pos_send.at[d], pos_recv.at[origin],
            lax.rem(me + d, members), group,
        )

    def kv_copy(j, origin):
        return remote(
            kv_stage.at[j], kv_buf.at[origin], kv_send.at[j], kv_recv.at[origin],
            mates * heads + kv_order[j], group,
        )

    def qg_copy(j, d, origin):
        source = qg_buf.at[me] if j == 0 else qg_stage.at[j]
        return remote(
            source, qg_buf.at[origin], qg_send.at[j, d], qg_recv.at[origin],
            lax.rem(mates + d, ratio) * heads + target(*near[j]), group,
        )

    for d in range(1, members):
        pos_copy(d, me).start()
    for j in range(1, heads):
        for copy in kv_locals[j]:
            copy.wait()
        kv_copy(j, mine).start()
    for j in range(heads):
        for copy in qg_locals[j]:
            copy.wait()
        for d in range(ratio):
            if j or d:
                qg_copy(j, d, me).start()

    dk_acc[...] = jnp.zeros_like(dk_acc)
    dv_acc[...] = jnp.zeros_like(dv_acc)
    pos_buf[me] = pos_mine[...]
    for d in range(1, members):
        pos_copy(d, lax.rem(me + members - d, members)).wait()

    def spread(i, carry):
        row = jnp.broadcast_to(
            pos_buf[mates * heads + i].astype(jnp.float32), (HEAD_DIM, width)
        )
        key_pos[i] = row.T[:rows]
        return carry

    lax.fori_loop(0, heads, spread, 0)
    for copy in kv_locals[0]:
        copy.wait()
    for j in range(1, heads):
        kv_copy(j, lax.rem(mine + heads - j, heads)).wait()

    def turn(i, carry):
        held = kv_buf[i, 0].astype(jnp.float32)
        key_t[i] = held.T.astype(jnp.bfloat16)
        return carry

    lax.fori_loop(0, heads, turn, 0)

    def unit_of(n):
        d = lax.rem(n, ratio)
        t = n // ratio
        return lax.rem(mates + d, ratio) * wide + lax.rem(place + t, wide)

    def operand(unit, a):
        return qg_buf[pl.ds(unit * pair, pair), a].reshape(block, HEAD_DIM)

    def tiles(values):
        return values.reshape(step * rows // 8, 8, block)

    def stat_copy(unit, d, origin):
        return remote(
            stat_buf.at[mates, unit], stat_buf.at[origin, unit],
            stat_send.at[d, unit], stat_recv.at[origin, unit],
            lax.rem(mates + d, ratio) * heads + mine, group,
        )

    def stats(n, outer):
        unit = unit_of(n)
        for c in range(pair):
            origin = unit * pair + c

            @pl.when(origin != me)
            def _():
                remote(
                    qg_buf.at[origin], qg_buf.at[origin], qg_send.at[0, 0], qg_recv.at[origin],
                    me, group,
                ).wait_recv()

        query, grad = operand(unit, 0), operand(unit, 1)
        rows_of = [pos_buf[unit * pair + c].astype(jnp.float32)[:, :rows] for c in range(pair)]
        pos_row = jnp.concatenate(rows_of, axis=1) if pair > 1 else rows_of[0]

        def one(s, carry):
            top, total, delta = carry
            held = pl.ds(s * step, step)
            key = kv_buf[held, 0].reshape(step * rows, HEAD_DIM)
            value = kv_buf[held, 1].reshape(step * rows, HEAD_DIM)
            scores = lax.dot_general(key, query, NT, preferred_element_type=jnp.float32)
            key_held = key_pos[held].reshape(step * rows, HEAD_DIM)
            key_held = jnp.concatenate([key_held] * (block // HEAD_DIM), axis=1)
            scores = jnp.where(key_held <= pos_row, scores, LOW)
            here = jnp.max(jnp.max(tiles(scores), axis=0), axis=0, keepdims=True)
            new_top = jnp.maximum(top, here)
            unscaled = jnp.exp2((scores - new_top) * sharp)
            probs = lax.dot_general(value, grad, NT, preferred_element_type=jnp.float32)
            z_buf[n, s] = unscaled
            p_buf[n, s] = probs
            tops[n, s] = jnp.broadcast_to(new_top, (8, block))
            alpha = jnp.exp2((top - new_top) * sharp)
            total = total * alpha + jnp.sum(tiles(unscaled), axis=0)
            delta = delta * alpha + jnp.sum(tiles(unscaled * probs), axis=0)
            return new_top, total, delta

        zero = jnp.zeros((8, block), jnp.float32)
        top, total, delta = lax.fori_loop(
            0, steps, one, (jnp.full((1, block), LOW, jnp.float32), zero, zero)
        )
        total = jnp.sum(total, axis=0, keepdims=True)
        delta = jnp.sum(delta, axis=0, keepdims=True)
        stat_buf[mates, unit] = jnp.concatenate(
            [top, total, delta, jnp.zeros((5, block), jnp.float32)], axis=0
        )
        for d in range(1, ratio):
            stat_copy(unit, d, mates).start()
        return outer

    lax.fori_loop(0, units, stats, 0)

    def grads(n, outer):
        unit = unit_of(n)
        for d in range(1, ratio):
            stat_copy(unit, d, lax.rem(mates + ratio - d, ratio)).wait()
        whole = [stat_buf[d, unit] for d in range(ratio)]
        top = functools.reduce(jnp.maximum, [w[0:1] for w in whole])
        shares = [jnp.exp2((w[0:1] - top) * sharp) for w in whole]
        inverse = 1.0 / functools.reduce(jnp.add, [w[1:2] * s for w, s in zip(whole, shares)])
        delta = functools.reduce(jnp.add, [w[2:3] * s for w, s in zip(whole, shares)]) * inverse
        query, grad = operand(unit, 0), operand(unit, 1)

        def one(s, query_t):
            held = pl.ds(s * step, step)
            factor = jnp.exp2((tops[n, s][0:1] - top) * sharp) * inverse
            weights = z_buf[n, s] * factor
            grad_scores = (weights * (p_buf[n, s] - delta)).astype(jnp.bfloat16)
            value_term = jnp.dot(
                weights.astype(jnp.bfloat16), grad, preferred_element_type=jnp.float32
            )
            key_term = jnp.dot(grad_scores, query, preferred_element_type=jnp.float32)
            dv_acc[held] += value_term.reshape(step, rows, HEAD_DIM)
            dk_acc[held] += key_term.reshape(step, rows, HEAD_DIM)
            for i in range(step):
                query_t = query_t + jnp.dot(
                    key_t[s * step + i], grad_scores[i * rows:(i + 1) * rows],
                    preferred_element_type=jnp.float32,
                )
            return query_t

        query_t = lax.fori_loop(0, steps, one, jnp.zeros((HEAD_DIM, block), jnp.float32))
        grad_query = (query_t * scaling).T.astype(jnp.bfloat16)
        grad_query = grad_query.reshape(pair, groups, part_rows, HEAD_DIM)
        dq_stage[unit] = grad_query
        for c in range(pair):
            for e in range(groups):
                owner = unit * pair + c
                other = lax.rem(group + e, groups)
                copy = remote(
                    dq_stage.at[unit, c, other], dq_back.at[mates, group * heads + mine],
                    dq_send.at[unit, c, e], dq_recv.at[mates, group * heads + mine],
                    owner, other,
                )
                if e:
                    copy.start()
                else:
                    pl.when(owner != me)(copy.start)
        return outer

    lax.fori_loop(0, units, grads, 0)

    dq_back[mates, group * heads + mine] = dq_stage[me // pair, core, group]

    def back_copy(j, origin):
        return remote(
            kv_final.at[j], kv_back.at[origin], back_send.at[j], back_recv.at[origin],
            mates * heads + kv_order[j], group,
        )

    for j in range(1, heads):
        kv_final[j, 0] = (dk_acc[kv_order[j]] * scaling).astype(jnp.bfloat16)
        kv_final[j, 1] = dv_acc[kv_order[j]].astype(jnp.bfloat16)
        back_copy(j, mine).start()
    kv_back[mine, 0] = (dk_acc[mine] * scaling).astype(jnp.bfloat16)
    kv_back[mine, 1] = dv_acc[mine].astype(jnp.bfloat16)

    for j in range(heads):
        for d in range(ratio):
            if j or d:
                qg_copy(j, d, me).wait_send()

    def dq_sent(unit, outer):
        for c in range(pair):
            for e in range(groups):
                owner = unit * pair + c
                other = lax.rem(group + e, groups)
                copy = remote(
                    dq_stage.at[unit, c, other], dq_back.at[mates, group * heads + mine],
                    dq_send.at[unit, c, e], dq_recv.at[mates, group * heads + mine],
                    owner, other,
                )
                if e:
                    copy.wait_send()
                else:
                    pl.when(owner != me)(copy.wait_send)
        return outer

    lax.fori_loop(0, units, dq_sent, 0)

    for d in range(ratio):
        for e in range(groups):
            for i in range(heads):
                giver = lax.rem(mates + d, ratio)
                slot = lax.rem(group + e, groups) * heads + lax.rem(mine + i, heads)
                if d or e or i:
                    remote(
                        dq_back.at[giver, slot], dq_back.at[giver, slot],
                        dq_send.at[0, 0, 0], dq_recv.at[giver, slot], me, group,
                    ).wait_recv()
    for h in range(groups * heads):
        parts = [dq_back[d, h].astype(jnp.float32) for d in range(ratio)]
        dq_out[:, h * HEAD_DIM:(h + 1) * HEAD_DIM] = functools.reduce(jnp.add, parts).astype(
            jnp.bfloat16
        )
    for j in range(1, heads):
        back_copy(j, lax.rem(mine + heads - j, heads)).wait()
    for h in range(heads):
        dk_out[:, h * HEAD_DIM:(h + 1) * HEAD_DIM] = kv_back[h, 0]
        dv_out[:, h * HEAD_DIM:(h + 1) * HEAD_DIM] = kv_back[h, 1]


def local(members, groups, query_rows, key_rows, value_rows, grad_output, positions):
    rows, wide = query_rows.shape
    heads = wide // HEAD_DIM
    ratio = members // heads
    width = -(-rows // HEAD_DIM) * HEAD_DIM
    pair = HEAD_DIM // math.gcd(rows, HEAD_DIM)
    step = math.gcd(heads, 2)
    units = members // pair
    block = pair * rows
    keys = heads * rows
    position_rows = jnp.pad(positions, (0, width - rows))[None]
    low, full = jnp.bfloat16, jnp.float32
    piece = (rows, HEAD_DIM)
    dma = pltpu.SemaphoreType.DMA
    scratch = [
        pltpu.VMEM((members, 2) + piece, low),
        pltpu.VMEM((heads, 2) + piece, low),
        pltpu.VMEM((heads, 2) + piece, low),
        pltpu.VMEM((heads, 2) + piece, low),
        pltpu.VMEM((heads, HEAD_DIM, rows), low),
        pltpu.VMEM((1, width), jnp.int32),
        pltpu.VMEM((members, 1, width), jnp.int32),
        pltpu.VMEM((heads,) + piece, full),
        pltpu.VMEM((units, heads // step, 8, block), full),
        pltpu.VMEM((units, heads // step, step * rows, block), full),
        pltpu.VMEM((units, heads // step, step * rows, block), full),
        pltpu.VMEM((heads,) + piece, full),
        pltpu.VMEM((heads,) + piece, full),
        pltpu.VMEM((ratio, units, 8, block), full),
        pltpu.VMEM((heads, 2) + piece, low),
        pltpu.VMEM((heads, 2) + piece, low),
        pltpu.VMEM((units, pair, groups, rows // groups, HEAD_DIM), low),
        pltpu.VMEM((ratio, groups * heads, rows // groups, HEAD_DIM), low),
        dma((2, heads)), dma((2, heads)), dma((heads, ratio)), dma((members,)),
        dma((heads,)), dma((heads,)), dma((members,)), dma((members,)),
        dma((ratio, units)), dma((ratio, units)), dma((heads,)), dma((heads,)),
        dma((units, pair, groups)), dma((ratio, groups * heads)),
    ]
    vmem = pl.BlockSpec(memory_space=pltpu.VMEM)
    hbm = pl.BlockSpec(memory_space=pl.ANY)
    return pl.pallas_call(
        functools.partial(kernel, members, heads, groups, rows, width, pair, step),
        out_shape=(
            jax.ShapeDtypeStruct((rows // groups, groups * wide), low),
            jax.ShapeDtypeStruct((rows, wide), low),
            jax.ShapeDtypeStruct((rows, wide), low),
        ),
        in_specs=[vmem, hbm, hbm, hbm, hbm],
        out_specs=(vmem, vmem, vmem),
        scratch_shapes=scratch,
        compiler_params=pltpu.CompilerParams(
            collective_id=0, has_side_effects=True, vmem_limit_bytes=63 * 1024 * 1024
        ),
    )(position_rows, query_rows, key_rows, value_rows, grad_output)


def solution(mesh):
    placed = (P("seq", "head"), P("seq", "head"), P("seq", "head"), P("seq", "head"), P("seq"))
    return jax.shard_map(
        functools.partial(local, mesh.shape["seq"], mesh.shape["head"]),
        mesh=mesh,
        in_specs=placed,
        out_specs=(P(("seq", "head"), None), P("seq", "head"), P("seq", "head")),
        check_vma=False,
    )
```

```python
import functools
import math

import jax
import jax.numpy as jnp
from jax import lax
from jax.experimental import pallas as pl
from jax.experimental.pallas import tpu as pltpu
from jax.sharding import PartitionSpec as P

HEAD_DIM = 128
MESH = pl.DeviceIdType.MESH
NT = (((1,), (1,)), ((), ()))
LOW = -1e30
PAIR = 2
STEP = 4
SEND_OUTER, SEND_INNER = "kCRh", "kCRh"
STATS_OUTER, STATS_INNER = "CRh", "CRh"
GRADS_OUTER, GRADS_INNER = "HCR", "RCH"
BACK_OUTER, BACK_INNER = "rC", "Cr"


def walk(order, sizes):
    found = [{}]
    for axis in order:
        values = list(range(sizes[axis.lower()]))
        if axis.isupper():
            values.reverse()
        found = [{**one, axis.lower(): v} for one in found for v in values]
    return found


def kernel(
    members, heads, groups, rows, width, pair, step,
    pos_ref, q_hbm, k_hbm, v_hbm, g_hbm,
    dq_out, dk_out, dv_out,
    qg_buf, kv_buf, qg_stage, kv_stage, key_t, pos_mine, pos_buf, key_pos, tops,
    z_buf, p_buf, dk_acc, dv_acc, stat_buf, kv_final, kv_back, dq_stage, dq_back,
    qg_local, kv_local, qg_send, qg_recv, kv_send, kv_recv, pos_send, pos_recv,
    stat_send, stat_recv, back_send, back_recv, dq_send, dq_recv,
):
    ratio = members // heads
    units = members // pair
    wide = heads // pair
    lines = 2 if wide % 2 == 0 else 1
    across = wide // lines
    sizes = {"h": ratio, "r": lines, "c": across, "k": 2}
    me = lax.axis_index("seq")
    group = lax.axis_index("head")
    mine = lax.rem(me, heads)
    mates = me // heads
    place = mine // pair
    core = lax.rem(mine, pair)
    line = place // across
    column = lax.rem(place, across)
    outer = (2 * mates < ratio) == (2 * line < lines)
    scaling = HEAD_DIM ** (-0.5)
    sharp = scaling / math.log(2.0)
    block = pair * rows
    steps = heads // step
    part_rows = rows // groups

    def by_row(act_outer, act_inner):
        pl.when(outer)(act_outer)
        pl.when(jnp.logical_not(outer))(act_inner)

    def columns(index):
        return pl.ds(pl.multiple_of(index * HEAD_DIM, HEAD_DIM), HEAD_DIM)

    others = [(r, c, e) for r in range(lines) for c in range(across) for e in range(pair)]

    def place_of(r, c):
        return lax.rem(line + r, lines) * across + lax.rem(column + c, across)

    def ahead(j):
        r, c, e = others[j]
        return place_of(r, c) * pair + lax.rem(core + e, pair)

    def behind(j):
        r, c, e = others[j]
        return place_of(lines - r, across - c) * pair + lax.rem(core + pair - e, pair)

    def local_copies(arrays, first, stage, sems, j):
        return [
            pltpu.make_async_copy(
                array.at[:, columns(ahead(j))], first.at[a] if j == 0 else stage.at[j, a],
                sems.at[a, j],
            )
            for a, array in enumerate(arrays)
        ]

    kv_locals = [
        local_copies((k_hbm, v_hbm), kv_buf.at[mine], kv_stage, kv_local, j)
        for j in range(heads)
    ]
    qg_locals = [
        local_copies((q_hbm, g_hbm), qg_buf.at[me], qg_stage, qg_local, j) for j in range(heads)
    ]
    for copies in kv_locals + qg_locals:
        for copy in copies:
            copy.start()

    pos_mine[...] = jnp.zeros_like(pos_mine)
    pos_mine[:, :rows] = pos_ref[...]
    barrier = pltpu.get_barrier_semaphore()
    for d in range(members):
        for e in range(groups):
            if d or e:
                pl.semaphore_signal(
                    barrier, inc=1,
                    device_id={
                        "seq": lax.rem(me + d, members), "head": lax.rem(group + e, groups),
                    },
                    device_id_type=MESH,
                )
    pl.semaphore_wait(barrier, members * groups - 1)

    def remote(source, sink, send, recv, seq, head):
        return pltpu.make_async_remote_copy(
            src_ref=source, dst_ref=sink, send_sem=send, recv_sem=recv,
            device_id={"seq": seq, "head": head}, device_id_type=MESH,
        )

    def pos_copy(d, origin):
        return remote(
            pos_mine, pos_buf.at[origin], pos_send.at[d], pos_recv.at[origin],
            lax.rem(me + d, members), group,
        )

    def kv_copy(j, origin):
        return remote(
            kv_stage.at[j], kv_buf.at[origin], kv_send.at[j], kv_recv.at[origin],
            mates * heads + ahead(j), group,
        )

    def qg_copy(j, d):
        source = qg_buf.at[me] if j == 0 else qg_stage.at[j]
        return remote(
            source, qg_buf.at[me], qg_send.at[j, d], qg_recv.at[me],
            lax.rem(mates + d, ratio) * heads + ahead(j), group,
        )

    for copies in kv_locals + qg_locals:
        for copy in copies:
            copy.wait()
    for d in range(1, members):
        pos_copy(d, me).start()

    def send_all(order):
        def act():
            for at in walk(order, sizes):
                for e in range(pair):
                    j = others.index((at["r"], at["c"], e))
                    if at["k"] == 0 and at["h"] == 0 and j:
                        kv_copy(j, mine).start()
                    if at["k"] == 1 and (at["h"] or j):
                        qg_copy(j, at["h"]).start()

        return act

    by_row(send_all(SEND_OUTER), send_all(SEND_INNER))

    dk_acc[...] = jnp.zeros_like(dk_acc)
    dv_acc[...] = jnp.zeros_like(dv_acc)
    pos_buf[me] = pos_mine[...]
    for d in range(1, members):
        pos_copy(d, lax.rem(me + members - d, members)).wait()

    def spread(i, carry):
        row = jnp.broadcast_to(
            pos_buf[mates * heads + i].astype(jnp.float32), (HEAD_DIM, width)
        )
        key_pos[i] = row.T[:rows]
        return carry

    lax.fori_loop(0, heads, spread, 0)
    for j in range(1, heads):
        kv_copy(j, behind(j)).wait()

    def turn(s, carry):
        held = kv_buf[pl.ds(s * step, step), 0].reshape(step * rows, HEAD_DIM)
        key_t[s] = held.astype(jnp.float32).T.astype(jnp.bfloat16)
        return carry

    lax.fori_loop(0, steps, turn, 0)

    def pick(table, k):
        value = jnp.int32(table[0])
        for i, entry in enumerate(table[1:]):
            value = jnp.where(k == i + 1, entry, value)
        return value

    def unit_of(k, order_outer, order_inner):
        tables = [
            [(at["h"] * lines + at["r"]) * across + at["c"] for at in walk(order, sizes)]
            for order in (order_outer, order_inner)
        ]
        n = jnp.where(outer, pick(tables[0], k), pick(tables[1], k))
        there = place_of(lax.rem(n // across, lines), lax.rem(n, across))
        return n, lax.rem(mates + n // wide, ratio) * wide + there

    def operand(unit, a):
        return qg_buf[pl.ds(unit * pair, pair), a].reshape(block, HEAD_DIM)

    def tiles(values):
        return values.reshape(step * rows // 8, 8, block)

    def stat_copy(unit, d, origin):
        return remote(
            stat_buf.at[mates, unit], stat_buf.at[origin, unit],
            stat_send.at[d, unit], stat_recv.at[origin, unit],
            lax.rem(mates + d, ratio) * heads + mine, group,
        )

    def stats(k, carried):
        n, unit = unit_of(k, STATS_OUTER, STATS_INNER)
        for c in range(pair):
            origin = unit * pair + c

            @pl.when(origin != me)
            def _():
                remote(
                    qg_buf.at[origin], qg_buf.at[origin], qg_send.at[0, 0], qg_recv.at[origin],
                    me, group,
                ).wait_recv()

        query, grad = operand(unit, 0), operand(unit, 1)
        rows_of = [pos_buf[unit * pair + c].astype(jnp.float32)[:, :rows] for c in range(pair)]
        pos_row = jnp.concatenate(rows_of, axis=1) if pair > 1 else rows_of[0]

        def one(s, carry):
            top, total, delta = carry
            held = pl.ds(s * step, step)
            key = kv_buf[held, 0].reshape(step * rows, HEAD_DIM)
            value = kv_buf[held, 1].reshape(step * rows, HEAD_DIM)
            scores = lax.dot_general(key, query, NT, preferred_element_type=jnp.float32)
            key_held = key_pos[held].reshape(step * rows, HEAD_DIM)
            key_held = jnp.concatenate([key_held] * (block // HEAD_DIM), axis=1)
            scores = jnp.where(key_held <= pos_row, scores, LOW)
            here = jnp.max(jnp.max(tiles(scores), axis=0), axis=0, keepdims=True)
            new_top = jnp.maximum(top, here)
            unscaled = jnp.exp2((scores - new_top) * sharp)
            probs = lax.dot_general(value, grad, NT, preferred_element_type=jnp.float32)
            z_buf[n, s] = unscaled
            p_buf[n, s] = probs
            tops[n, s] = jnp.broadcast_to(new_top, (8, block))
            alpha = jnp.exp2((top - new_top) * sharp)
            total = total * alpha + jnp.sum(tiles(unscaled), axis=0)
            delta = delta * alpha + jnp.sum(tiles(unscaled * probs), axis=0)
            return new_top, total, delta

        zero = jnp.zeros((8, block), jnp.float32)
        top, total, delta = lax.fori_loop(
            0, steps, one, (jnp.full((1, block), LOW, jnp.float32), zero, zero)
        )
        total = jnp.sum(total, axis=0, keepdims=True)
        delta = jnp.sum(delta, axis=0, keepdims=True)
        stat_buf[mates, unit] = jnp.concatenate(
            [top, total, delta, jnp.zeros((5, block), jnp.float32)], axis=0
        )
        for d in range(1, ratio):
            stat_copy(unit, d, mates).start()
        return carried

    lax.fori_loop(0, units, stats, 0)

    def grads(k, carried):
        n, unit = unit_of(k, GRADS_OUTER, GRADS_INNER)
        for d in range(1, ratio):
            stat_copy(unit, d, lax.rem(mates + ratio - d, ratio)).wait()
        whole = [stat_buf[d, unit] for d in range(ratio)]
        top = functools.reduce(jnp.maximum, [w[0:1] for w in whole])
        shares = [jnp.exp2((w[0:1] - top) * sharp) for w in whole]
        inverse = 1.0 / functools.reduce(jnp.add, [w[1:2] * s for w, s in zip(whole, shares)])
        delta = functools.reduce(jnp.add, [w[2:3] * s for w, s in zip(whole, shares)]) * inverse
        query, grad = operand(unit, 0), operand(unit, 1)

        def one(s, query_t):
            held = pl.ds(s * step, step)
            factor = jnp.exp2((tops[n, s][0:1] - top) * sharp) * inverse
            weights = z_buf[n, s] * factor
            grad_scores = (weights * (p_buf[n, s] - delta)).astype(jnp.bfloat16)
            value_term = jnp.dot(
                weights.astype(jnp.bfloat16), grad, preferred_element_type=jnp.float32
            )
            key_term = jnp.dot(grad_scores, query, preferred_element_type=jnp.float32)
            dv_acc[held] += value_term.reshape(step, rows, HEAD_DIM)
            dk_acc[held] += key_term.reshape(step, rows, HEAD_DIM)
            return query_t + jnp.dot(
                key_t[s], grad_scores, preferred_element_type=jnp.float32
            )

        query_t = lax.fori_loop(0, steps, one, jnp.zeros((HEAD_DIM, block), jnp.float32))
        grad_query = (query_t * scaling).T.astype(jnp.bfloat16)
        grad_query = grad_query.reshape(pair, groups, part_rows, HEAD_DIM)
        dq_stage[unit] = grad_query
        for c in range(pair):
            for e in range(groups):
                owner = unit * pair + c
                other = lax.rem(group + e, groups)
                copy = remote(
                    dq_stage.at[unit, c, other], dq_back.at[mates, group * heads + mine],
                    dq_send.at[unit, c, e], dq_recv.at[mates, group * heads + mine],
                    owner, other,
                )
                if e:
                    copy.start()
                else:
                    pl.when(owner != me)(copy.start)
        return carried

    lax.fori_loop(0, units, grads, 0)

    dq_back[mates, group * heads + mine] = dq_stage[me // pair, core, group]

    def back_copy(j, origin):
        return remote(
            kv_final.at[j], kv_back.at[origin], back_send.at[j], back_recv.at[origin],
            mates * heads + ahead(j), group,
        )

    def give_back(order):
        def act():
            for at in walk(order, sizes):
                for e in range(pair):
                    j = others.index((at["r"], at["c"], e))
                    if j:
                        kv_final[j, 0] = (dk_acc[ahead(j)] * scaling).astype(jnp.bfloat16)
                        kv_final[j, 1] = dv_acc[ahead(j)].astype(jnp.bfloat16)
                        back_copy(j, mine).start()

        return act

    by_row(give_back(BACK_OUTER), give_back(BACK_INNER))
    kv_back[mine, 0] = (dk_acc[mine] * scaling).astype(jnp.bfloat16)
    kv_back[mine, 1] = dv_acc[mine].astype(jnp.bfloat16)

    for j in range(heads):
        for d in range(ratio):
            if j or d:
                qg_copy(j, d).wait_send()

    def dq_sent(unit, carried):
        for c in range(pair):
            for e in range(groups):
                owner = unit * pair + c
                other = lax.rem(group + e, groups)
                copy = remote(
                    dq_stage.at[unit, c, other], dq_back.at[mates, group * heads + mine],
                    dq_send.at[unit, c, e], dq_recv.at[mates, group * heads + mine],
                    owner, other,
                )
                if e:
                    copy.wait_send()
                else:
                    pl.when(owner != me)(copy.wait_send)
        return carried

    lax.fori_loop(0, units, dq_sent, 0)

    for d in range(ratio):
        for e in range(groups):
            for i in range(heads):
                giver = lax.rem(mates + d, ratio)
                slot = lax.rem(group + e, groups) * heads + lax.rem(mine + i, heads)
                if d or e or i:
                    remote(
                        dq_back.at[giver, slot], dq_back.at[giver, slot],
                        dq_send.at[0, 0, 0], dq_recv.at[giver, slot], me, group,
                    ).wait_recv()
    for h in range(groups * heads):
        parts = [dq_back[d, h].astype(jnp.float32) for d in range(ratio)]
        dq_out[:, h * HEAD_DIM:(h + 1) * HEAD_DIM] = functools.reduce(jnp.add, parts).astype(
            jnp.bfloat16
        )
    for j in range(1, heads):
        back_copy(j, behind(j)).wait()
    for h in range(heads):
        dk_out[:, h * HEAD_DIM:(h + 1) * HEAD_DIM] = kv_back[h, 0]
        dv_out[:, h * HEAD_DIM:(h + 1) * HEAD_DIM] = kv_back[h, 1]


def local(members, groups, query_rows, key_rows, value_rows, grad_output, positions):
    rows, wide = query_rows.shape
    heads = wide // HEAD_DIM
    ratio = members // heads
    width = -(-rows // HEAD_DIM) * HEAD_DIM
    pair = math.gcd(heads, PAIR)
    step = math.gcd(heads, STEP)
    units = members // pair
    block = pair * rows
    position_rows = positions[None]
    low, full = jnp.bfloat16, jnp.float32
    piece = (rows, HEAD_DIM)
    dma = pltpu.SemaphoreType.DMA
    scratch = [
        pltpu.VMEM((members, 2) + piece, low),
        pltpu.VMEM((heads, 2) + piece, low),
        pltpu.VMEM((heads, 2) + piece, low),
        pltpu.VMEM((heads, 2) + piece, low),
        pltpu.VMEM((heads // step, HEAD_DIM, step * rows), low),
        pltpu.VMEM((1, width), jnp.int32),
        pltpu.VMEM((members, 1, width), jnp.int32),
        pltpu.VMEM((heads,) + piece, full),
        pltpu.VMEM((units, heads // step, 8, block), full),
        pltpu.VMEM((units, heads // step, step * rows, block), full),
        pltpu.VMEM((units, heads // step, step * rows, block), full),
        pltpu.VMEM((heads,) + piece, full),
        pltpu.VMEM((heads,) + piece, full),
        pltpu.VMEM((ratio, units, 8, block), full),
        pltpu.VMEM((heads, 2) + piece, low),
        pltpu.VMEM((heads, 2) + piece, low),
        pltpu.VMEM((units, pair, groups, rows // groups, HEAD_DIM), low),
        pltpu.VMEM((ratio, groups * heads, rows // groups, HEAD_DIM), low),
        dma((2, heads)), dma((2, heads)), dma((heads, ratio)), dma((members,)),
        dma((heads,)), dma((heads,)), dma((members,)), dma((members,)),
        dma((ratio, units)), dma((ratio, units)), dma((heads,)), dma((heads,)),
        dma((units, pair, groups)), dma((ratio, groups * heads)),
    ]
    vmem = pl.BlockSpec(memory_space=pltpu.VMEM)
    hbm = pl.BlockSpec(memory_space=pl.ANY)
    return pl.pallas_call(
        functools.partial(kernel, members, heads, groups, rows, width, pair, step),
        out_shape=(
            jax.ShapeDtypeStruct((rows // groups, groups * wide), low),
            jax.ShapeDtypeStruct((rows, wide), low),
            jax.ShapeDtypeStruct((rows, wide), low),
        ),
        in_specs=[vmem, hbm, hbm, hbm, hbm],
        out_specs=(vmem, vmem, vmem),
        scratch_shapes=scratch,
        compiler_params=pltpu.CompilerParams(
            collective_id=0, has_side_effects=True, vmem_limit_bytes=63 * 1024 * 1024
        ),
    )(position_rows, query_rows, key_rows, value_rows, grad_output)


def solution(mesh):
    placed = (P("seq", "head"), P("seq", "head"), P("seq", "head"), P("seq", "head"), P("seq"))
    return jax.shard_map(
        functools.partial(local, mesh.shape["seq"], mesh.shape["head"]),
        mesh=mesh,
        in_specs=placed,
        out_specs=(P(("seq", "head"), None), P("seq", "head"), P("seq", "head")),
        check_vma=False,
    )
```

```python
import functools
import math

import jax
import jax.numpy as jnp
from jax import lax
from jax.experimental import pallas as pl
from jax.experimental.pallas import tpu as pltpu
from jax.sharding import PartitionSpec as P

HEAD_DIM = 128
MESH = pl.DeviceIdType.MESH
NT = (((1,), (1,)), ((), ()))
LOW = -1e30
PAIR = 2
STEP = 4
SEND_OUTER, SEND_INNER = "kCRh", "kCRh"
STATS_OUTER, STATS_INNER = "CRh", "CRh"
GRADS_OUTER, GRADS_INNER = "HCR", "RCH"
BACK_OUTER, BACK_INNER = "rC", "Cr"


def walk(order, sizes):
    found = [{}]
    for axis in order:
        values = list(range(sizes[axis.lower()]))
        if axis.isupper():
            values.reverse()
        found = [{**one, axis.lower(): v} for one in found for v in values]
    return found


def kernel(
    members, heads, groups, rows, width, pair, step,
    pos_ref, q_hbm, k_hbm, v_hbm, g_hbm,
    dq_out, dk_out, dv_out,
    qg_buf, kv_buf, qg_stage, kv_stage, key_t, pos_mine, pos_buf, key_pos, tops,
    z_buf, p_buf, dk_acc, dv_acc, stat_buf, kv_final, dq_stage, dq_back, dq_sum,
    qg_local, kv_local, qg_send, qg_recv, kv_send, kv_recv, pos_send, pos_recv,
    stat_send, stat_recv, back_send, back_recv, back_own, dq_send, dq_recv, dq_own,
):
    ratio = members // heads
    units = members // pair
    wide = heads // pair
    lines = 2 if wide % 2 == 0 else 1
    across = wide // lines
    sizes = {"h": ratio, "r": lines, "c": across, "k": 2}
    me = lax.axis_index("seq")
    group = lax.axis_index("head")
    mine = lax.rem(me, heads)
    mates = me // heads
    place = mine // pair
    core = lax.rem(mine, pair)
    line = place // across
    column = lax.rem(place, across)
    outer = (2 * mates < ratio) == (2 * line < lines)
    scaling = HEAD_DIM ** (-0.5)
    sharp = scaling / math.log(2.0)
    block = pair * rows
    steps = heads // step
    part_rows = rows // groups

    def by_row(act_outer, act_inner):
        pl.when(outer)(act_outer)
        pl.when(jnp.logical_not(outer))(act_inner)

    def columns(index):
        return pl.ds(pl.multiple_of(index * HEAD_DIM, HEAD_DIM), HEAD_DIM)

    others = [(r, c, e) for r in range(lines) for c in range(across) for e in range(pair)]

    def place_of(r, c):
        return lax.rem(line + r, lines) * across + lax.rem(column + c, across)

    def ahead(j):
        r, c, e = others[j]
        return place_of(r, c) * pair + lax.rem(core + e, pair)

    def behind(j):
        r, c, e = others[j]
        return place_of(lines - r, across - c) * pair + lax.rem(core + pair - e, pair)

    def local_copies(arrays, first, stage, sems, j):
        return [
            pltpu.make_async_copy(
                array.at[:, columns(ahead(j))], first.at[a] if j == 0 else stage.at[j, a],
                sems.at[a, j],
            )
            for a, array in enumerate(arrays)
        ]

    kv_locals = [
        local_copies((k_hbm, v_hbm), kv_buf.at[mine], kv_stage, kv_local, j)
        for j in range(heads)
    ]
    qg_locals = [
        local_copies((q_hbm, g_hbm), qg_buf.at[me], qg_stage, qg_local, j) for j in range(heads)
    ]
    for copies in kv_locals + qg_locals:
        for copy in copies:
            copy.start()

    pos_mine[...] = jnp.zeros_like(pos_mine)
    pos_mine[:, :rows] = pos_ref[...]
    barrier = pltpu.get_barrier_semaphore()
    for d in range(members):
        for e in range(groups):
            if d or e:
                pl.semaphore_signal(
                    barrier, inc=1,
                    device_id={
                        "seq": lax.rem(me + d, members), "head": lax.rem(group + e, groups),
                    },
                    device_id_type=MESH,
                )
    pl.semaphore_wait(barrier, members * groups - 1)

    def remote(source, sink, send, recv, seq, head):
        return pltpu.make_async_remote_copy(
            src_ref=source, dst_ref=sink, send_sem=send, recv_sem=recv,
            device_id={"seq": seq, "head": head}, device_id_type=MESH,
        )

    def pos_copy(d, origin):
        return remote(
            pos_mine, pos_buf.at[origin], pos_send.at[d], pos_recv.at[origin],
            lax.rem(me + d, members), group,
        )

    def kv_copy(j, origin):
        return remote(
            kv_stage.at[j], kv_buf.at[origin], kv_send.at[j], kv_recv.at[origin],
            mates * heads + ahead(j), group,
        )

    def qg_copy(j, d):
        source = qg_buf.at[me] if j == 0 else qg_stage.at[j]
        return remote(
            source, qg_buf.at[me], qg_send.at[j, d], qg_recv.at[me],
            lax.rem(mates + d, ratio) * heads + ahead(j), group,
        )

    for copies in kv_locals + qg_locals:
        for copy in copies:
            copy.wait()
    for d in range(1, members):
        pos_copy(d, me).start()

    def send_all(order):
        def act():
            for at in walk(order, sizes):
                for e in range(pair):
                    j = others.index((at["r"], at["c"], e))
                    if at["k"] == 0 and at["h"] == 0 and j:
                        kv_copy(j, mine).start()
                    if at["k"] == 1 and (at["h"] or j):
                        qg_copy(j, at["h"]).start()

        return act

    by_row(send_all(SEND_OUTER), send_all(SEND_INNER))

    dk_acc[...] = jnp.zeros_like(dk_acc)
    dv_acc[...] = jnp.zeros_like(dv_acc)
    pos_buf[me] = pos_mine[...]
    for d in range(1, members):
        pos_copy(d, lax.rem(me + members - d, members)).wait()

    def spread(i, carry):
        row = jnp.broadcast_to(
            pos_buf[mates * heads + i].astype(jnp.float32), (HEAD_DIM, width)
        )
        key_pos[i] = row.T[:rows]
        return carry

    lax.fori_loop(0, heads, spread, 0)
    for j in range(1, heads):
        kv_copy(j, behind(j)).wait()

    def turn(s, carry):
        held = kv_buf[pl.ds(s * step, step), 0].reshape(step * rows, HEAD_DIM)
        key_t[s] = held.astype(jnp.float32).T.astype(jnp.bfloat16)
        return carry

    lax.fori_loop(0, steps, turn, 0)

    def pick(table, k):
        value = jnp.int32(table[0])
        for i, entry in enumerate(table[1:]):
            value = jnp.where(k == i + 1, entry, value)
        return value

    def unit_of(k, order_outer, order_inner):
        tables = [
            [(at["h"] * lines + at["r"]) * across + at["c"] for at in walk(order, sizes)]
            for order in (order_outer, order_inner)
        ]
        n = jnp.where(outer, pick(tables[0], k), pick(tables[1], k))
        there = place_of(lax.rem(n // across, lines), lax.rem(n, across))
        return n, lax.rem(mates + n // wide, ratio) * wide + there

    def operand(unit, a):
        return qg_buf[pl.ds(unit * pair, pair), a].reshape(block, HEAD_DIM)

    def tiles(values):
        return values.reshape(step * rows // 8, 8, block)

    def stat_copy(unit, d, origin):
        return remote(
            stat_buf.at[mates, unit], stat_buf.at[origin, unit],
            stat_send.at[d, unit], stat_recv.at[origin, unit],
            lax.rem(mates + d, ratio) * heads + mine, group,
        )

    def stats(k, carried):
        n, unit = unit_of(k, STATS_OUTER, STATS_INNER)
        for c in range(pair):
            origin = unit * pair + c

            @pl.when(origin != me)
            def _():
                remote(
                    qg_buf.at[origin], qg_buf.at[origin], qg_send.at[0, 0], qg_recv.at[origin],
                    me, group,
                ).wait_recv()

        query, grad = operand(unit, 0), operand(unit, 1)
        rows_of = [pos_buf[unit * pair + c].astype(jnp.float32)[:, :rows] for c in range(pair)]
        pos_row = jnp.concatenate(rows_of, axis=1) if pair > 1 else rows_of[0]

        def one(s, carry):
            top, total, delta = carry
            held = pl.ds(s * step, step)
            key = kv_buf[held, 0].reshape(step * rows, HEAD_DIM)
            value = kv_buf[held, 1].reshape(step * rows, HEAD_DIM)
            scores = lax.dot_general(key, query, NT, preferred_element_type=jnp.float32)
            key_held = key_pos[held].reshape(step * rows, HEAD_DIM)
            key_held = jnp.concatenate([key_held] * (block // HEAD_DIM), axis=1)
            scores = jnp.where(key_held <= pos_row, scores, LOW)
            here = jnp.max(jnp.max(tiles(scores), axis=0), axis=0, keepdims=True)
            new_top = jnp.maximum(top, here)
            unscaled = jnp.exp2((scores - new_top) * sharp)
            probs = lax.dot_general(value, grad, NT, preferred_element_type=jnp.float32)
            z_buf[n, s] = unscaled
            p_buf[n, s] = probs
            tops[n, s] = jnp.broadcast_to(new_top, (8, block))
            alpha = jnp.exp2((top - new_top) * sharp)
            total = total * alpha + jnp.sum(tiles(unscaled), axis=0)
            delta = delta * alpha + jnp.sum(tiles(unscaled * probs), axis=0)
            return new_top, total, delta

        zero = jnp.zeros((8, block), jnp.float32)
        top, total, delta = lax.fori_loop(
            0, steps, one, (jnp.full((1, block), LOW, jnp.float32), zero, zero)
        )
        total = jnp.sum(total, axis=0, keepdims=True)
        delta = jnp.sum(delta, axis=0, keepdims=True)
        stat_buf[mates, unit] = jnp.concatenate(
            [top, total, delta, jnp.zeros((5, block), jnp.float32)], axis=0
        )
        for d in range(1, ratio):
            stat_copy(unit, d, mates).start()
        return carried

    lax.fori_loop(0, units, stats, 0)

    def grads(k, carried):
        n, unit = unit_of(k, GRADS_OUTER, GRADS_INNER)
        for d in range(1, ratio):
            stat_copy(unit, d, lax.rem(mates + ratio - d, ratio)).wait()
        whole = [stat_buf[d, unit] for d in range(ratio)]
        top = functools.reduce(jnp.maximum, [w[0:1] for w in whole])
        shares = [jnp.exp2((w[0:1] - top) * sharp) for w in whole]
        inverse = 1.0 / functools.reduce(jnp.add, [w[1:2] * s for w, s in zip(whole, shares)])
        delta = functools.reduce(jnp.add, [w[2:3] * s for w, s in zip(whole, shares)]) * inverse
        query, grad = operand(unit, 0), operand(unit, 1)

        def one(s, query_t):
            held = pl.ds(s * step, step)
            factor = jnp.exp2((tops[n, s][0:1] - top) * sharp) * inverse
            weights = z_buf[n, s] * factor
            grad_scores = (weights * (p_buf[n, s] - delta)).astype(jnp.bfloat16)
            value_term = jnp.dot(
                weights.astype(jnp.bfloat16), grad, preferred_element_type=jnp.float32
            )
            key_term = jnp.dot(grad_scores, query, preferred_element_type=jnp.float32)
            dv_acc[held] += value_term.reshape(step, rows, HEAD_DIM)
            dk_acc[held] += key_term.reshape(step, rows, HEAD_DIM)
            return query_t + jnp.dot(
                key_t[s], grad_scores, preferred_element_type=jnp.float32
            )

        query_t = lax.fori_loop(0, steps, one, jnp.zeros((HEAD_DIM, block), jnp.float32))
        grad_query = (query_t * scaling).T.astype(jnp.bfloat16)
        grad_query = grad_query.reshape(pair, groups, part_rows, HEAD_DIM)
        dq_stage[unit] = grad_query
        for c in range(pair):
            for e in range(groups):
                owner = unit * pair + c
                other = lax.rem(group + e, groups)
                copy = remote(
                    dq_stage.at[unit, c, other], dq_back.at[mates, group * heads + mine],
                    dq_send.at[unit, c, e], dq_recv.at[mates, group * heads + mine],
                    owner, other,
                )
                if e:
                    copy.start()
                else:
                    pl.when(owner != me)(copy.start)
        return carried

    lax.fori_loop(0, units, grads, 0)

    dq_back[mates, group * heads + mine] = dq_stage[me // pair, core, group]

    def back_copies(j, origin):
        return [
            remote(
                kv_final.at[j, a], out.at[:, columns(origin)], back_send.at[a, j],
                back_recv.at[a, origin], mates * heads + ahead(j), group,
            )
            for a, out in enumerate((dk_out, dv_out))
        ]

    def finish(j):
        kv_final[j, 0] = (dk_acc[ahead(j)] * scaling).astype(jnp.bfloat16)
        kv_final[j, 1] = dv_acc[ahead(j)].astype(jnp.bfloat16)

    def give_back(order):
        def act():
            for at in walk(order, sizes):
                for e in range(pair):
                    j = others.index((at["r"], at["c"], e))
                    if j:
                        finish(j)
                        for copy in back_copies(j, mine):
                            copy.start()

        return act

    by_row(give_back(BACK_OUTER), give_back(BACK_INNER))
    finish(0)
    back_locals = [
        pltpu.make_async_copy(kv_final.at[0, a], out.at[:, columns(mine)], back_own.at[a])
        for a, out in enumerate((dk_out, dv_out))
    ]
    for copy in back_locals:
        copy.start()

    for j in range(heads):
        for d in range(ratio):
            if j or d:
                qg_copy(j, d).wait_send()

    def dq_sent(unit, carried):
        for c in range(pair):
            for e in range(groups):
                owner = unit * pair + c
                other = lax.rem(group + e, groups)
                copy = remote(
                    dq_stage.at[unit, c, other], dq_back.at[mates, group * heads + mine],
                    dq_send.at[unit, c, e], dq_recv.at[mates, group * heads + mine],
                    owner, other,
                )
                if e:
                    copy.wait_send()
                else:
                    pl.when(owner != me)(copy.wait_send)
        return carried

    lax.fori_loop(0, units, dq_sent, 0)

    for d in range(ratio):
        for e in range(groups):
            for i in range(heads):
                giver = lax.rem(mates + d, ratio)
                slot = lax.rem(group + e, groups) * heads + lax.rem(mine + i, heads)
                if d or e or i:
                    remote(
                        dq_back.at[giver, slot], dq_back.at[giver, slot],
                        dq_send.at[0, 0, 0], dq_recv.at[giver, slot], me, group,
                    ).wait_recv()
    for h in range(groups * heads):
        parts = [dq_back[d, h].astype(jnp.float32) for d in range(ratio)]
        dq_sum[:, h * HEAD_DIM:(h + 1) * HEAD_DIM] = functools.reduce(jnp.add, parts).astype(
            jnp.bfloat16
        )
    dq_local = pltpu.make_async_copy(dq_sum, dq_out, dq_own)
    dq_local.start()
    for j in range(1, heads):
        for copy in back_copies(j, behind(j)):
            copy.wait()
    for copy in back_locals + [dq_local]:
        copy.wait()


def settle(a_in, b_in, c_in, a_out, b_out, c_out, a_mid, b_mid, c_mid, come, go):
    ins = [
        pltpu.make_async_copy(source, middle, come.at[i])
        for i, (source, middle) in enumerate(((a_in, a_mid), (b_in, b_mid), (c_in, c_mid)))
    ]
    outs = [
        pltpu.make_async_copy(middle, sink, go.at[i])
        for i, (middle, sink) in enumerate(((a_mid, a_out), (b_mid, b_out), (c_mid, c_out)))
    ]
    for copy in ins:
        copy.start()
    for copy, then in zip(ins, outs):
        copy.wait()
        then.start()
    for copy in outs:
        copy.wait()


def local(members, groups, query_rows, key_rows, value_rows, grad_output, positions):
    rows, wide = query_rows.shape
    heads = wide // HEAD_DIM
    ratio = members // heads
    width = -(-rows // HEAD_DIM) * HEAD_DIM
    pair = math.gcd(heads, PAIR)
    step = math.gcd(heads, STEP)
    units = members // pair
    block = pair * rows
    position_rows = positions[None]
    low, full = jnp.bfloat16, jnp.float32
    piece = (rows, HEAD_DIM)
    dma = pltpu.SemaphoreType.DMA
    scratch = [
        pltpu.VMEM((members, 2) + piece, low),
        pltpu.VMEM((heads, 2) + piece, low),
        pltpu.VMEM((heads, 2) + piece, low),
        pltpu.VMEM((heads, 2) + piece, low),
        pltpu.VMEM((heads // step, HEAD_DIM, step * rows), low),
        pltpu.VMEM((1, width), jnp.int32),
        pltpu.VMEM((members, 1, width), jnp.int32),
        pltpu.VMEM((heads,) + piece, full),
        pltpu.VMEM((units, heads // step, 8, block), full),
        pltpu.VMEM((units, heads // step, step * rows, block), full),
        pltpu.VMEM((units, heads // step, step * rows, block), full),
        pltpu.VMEM((heads,) + piece, full),
        pltpu.VMEM((heads,) + piece, full),
        pltpu.VMEM((ratio, units, 8, block), full),
        pltpu.VMEM((heads, 2) + piece, low),
        pltpu.VMEM((units, pair, groups, rows // groups, HEAD_DIM), low),
        pltpu.VMEM((ratio, groups * heads, rows // groups, HEAD_DIM), low),
        pltpu.VMEM((rows // groups, groups * wide), low),
        dma((2, heads)), dma((2, heads)), dma((heads, ratio)), dma((members,)),
        dma((heads,)), dma((heads,)), dma((members,)), dma((members,)),
        dma((ratio, units)), dma((ratio, units)), dma((2, heads)), dma((2, heads)), dma((2,)),
        dma((units, pair, groups)), dma((ratio, groups * heads)), dma,
    ]
    vmem = pl.BlockSpec(memory_space=pltpu.VMEM)
    hbm = pl.BlockSpec(memory_space=pl.ANY)
    results = pl.pallas_call(
        functools.partial(kernel, members, heads, groups, rows, width, pair, step),
        out_shape=(
            jax.ShapeDtypeStruct((rows // groups, groups * wide), low),
            jax.ShapeDtypeStruct((rows, wide), low),
            jax.ShapeDtypeStruct((rows, wide), low),
        ),
        in_specs=[vmem, hbm, hbm, hbm, hbm],
        out_specs=(hbm, hbm, hbm),
        scratch_shapes=scratch,
        compiler_params=pltpu.CompilerParams(
            collective_id=0, has_side_effects=True, vmem_limit_bytes=63 * 1024 * 1024
        ),
    )(position_rows, query_rows, key_rows, value_rows, grad_output)
    return pl.pallas_call(
        settle,
        out_shape=tuple(jax.ShapeDtypeStruct(r.shape, r.dtype) for r in results),
        in_specs=[hbm, hbm, hbm],
        out_specs=(hbm, hbm, hbm),
        scratch_shapes=[pltpu.VMEM(r.shape, r.dtype) for r in results] + [dma((3,)), dma((3,))],
    )(*results)


def solution(mesh):
    placed = (P("seq", "head"), P("seq", "head"), P("seq", "head"), P("seq", "head"), P("seq"))
    return jax.shard_map(
        functools.partial(local, mesh.shape["seq"], mesh.shape["head"]),
        mesh=mesh,
        in_specs=placed,
        out_specs=(P(("seq", "head"), None), P("seq", "head"), P("seq", "head")),
        check_vma=False,
    )
```

```python
import functools
import math

import jax
import jax.numpy as jnp
from jax import lax
from jax.experimental import pallas as pl
from jax.experimental.pallas import tpu as pltpu
from jax.sharding import PartitionSpec as P

HEAD_DIM = 128
MESH = pl.DeviceIdType.MESH
NT = (((1,), (1,)), ((), ()))
LOW = -1e30
LAG = 6
PAIR = 2
STEP = 4
SEND_OUTER, SEND_INNER = "kCRh", "kCRh"
STATS_OUTER, STATS_INNER = ".CRh", ".CRh"
GRADS_OUTER, GRADS_INNER = "CRH", "CRH"
BACK_OUTER, BACK_INNER = "RC", "RC"


def walk(order, sizes):
    found = [{}]
    for axis in order:
        values = list(range(sizes[axis.lower()]))
        if axis.isupper():
            values.reverse()
        found = [{**one, axis.lower(): v} for one in found for v in values]
    return found


def kernel(
    members, heads, groups, rows, width, pair, step,
    pos_ref, q_hbm, k_hbm, v_hbm, g_hbm,
    dq_out, dk_out, dv_out,
    qg_buf, kv_buf, qg_stage, kv_stage, key_t, pos_mine, pos_buf, key_pos, tops,
    z_buf, p_buf, dk_acc, dv_acc, stat_buf, kv_final, dq_stage, dq_back, dq_sum,
    qg_local, kv_local, qg_send, qg_recv, kv_send, kv_recv, pos_send, pos_recv,
    stat_send, stat_recv, back_send, back_recv, back_own, dq_send, dq_recv, dq_own,
):
    ratio = members // heads
    units = members // pair
    wide = heads // pair
    lines = 2 if wide % 2 == 0 else 1
    across = wide // lines
    sizes = {"h": ratio, "r": lines, "c": across, "k": 2}
    me = lax.axis_index("seq")
    group = lax.axis_index("head")
    mine = lax.rem(me, heads)
    mates = me // heads
    place = mine // pair
    core = lax.rem(mine, pair)
    line = place // across
    column = lax.rem(place, across)
    outer = (2 * mates < ratio) == (2 * line < lines)
    scaling = HEAD_DIM ** (-0.5)
    sharp = scaling / math.log(2.0)
    slot = (mates * groups + group) * heads + mine
    block = pair * rows
    steps = heads // step
    part_rows = rows // groups

    barrier = pltpu.get_barrier_semaphore()
    for d in range(members):
        for e in range(groups):
            if d or e:
                pl.semaphore_signal(
                    barrier, inc=1,
                    device_id={
                        "seq": lax.rem(me + d, members), "head": lax.rem(group + e, groups),
                    },
                    device_id_type=MESH,
                )

    def by_row(act_outer, act_inner):
        pl.when(outer)(act_outer)
        pl.when(jnp.logical_not(outer))(act_inner)

    def columns(index):
        return pl.ds(pl.multiple_of(index * HEAD_DIM, HEAD_DIM), HEAD_DIM)

    others = [(r, c, e) for r in range(lines) for c in range(across) for e in range(pair)]

    def place_of(r, c):
        return lax.rem(line + r, lines) * across + lax.rem(column + c, across)

    def ahead(j):
        r, c, e = others[j]
        return place_of(r, c) * pair + lax.rem(core + e, pair)

    def behind(j):
        r, c, e = others[j]
        return place_of(lines - r, across - c) * pair + lax.rem(core + pair - e, pair)

    def local_copies(arrays, first, stage, sems, j):
        return [
            pltpu.make_async_copy(
                array.at[:, columns(ahead(j))], first.at[a] if j == 0 else stage.at[j, a],
                sems,
            )
            for a, array in enumerate(arrays)
        ]

    kv_locals = [
        local_copies((k_hbm, v_hbm), kv_buf.at[mine], kv_stage, kv_local, j)
        for j in range(heads)
    ]
    qg_locals = [
        local_copies((q_hbm, g_hbm), qg_buf.at[me], qg_stage, qg_local, j) for j in range(heads)
    ]
    for copies in kv_locals + qg_locals:
        for copy in copies:
            copy.start()

    pos_mine[...] = jnp.zeros_like(pos_mine)
    pos_mine[:, :rows] = pos_ref[...]
    pl.semaphore_wait(barrier, members * groups - 1)

    def remote(source, sink, send, recv, seq, head):
        return pltpu.make_async_remote_copy(
            src_ref=source, dst_ref=sink, send_sem=send, recv_sem=recv,
            device_id={"seq": seq, "head": head}, device_id_type=MESH,
        )

    def pos_copy(d, origin):
        return remote(
            pos_mine, pos_buf.at[origin], pos_send, pos_recv,
            lax.rem(me + d, members), group,
        )

    def kv_copy(j, origin):
        return remote(
            kv_stage.at[j], kv_buf.at[origin], kv_send, kv_recv,
            mates * heads + ahead(j), group,
        )

    def qg_copy(j, d):
        source = qg_buf.at[me] if j == 0 else qg_stage.at[j]
        return remote(
            source, qg_buf.at[me], qg_send, qg_recv.at[me],
            lax.rem(mates + d, ratio) * heads + ahead(j), group,
        )

    def settled(ref, sem):
        remote(ref, ref, sem, sem, me, group).wait_recv()

    settled(kv_stage, kv_local)
    settled(qg_stage, qg_local)
    for d in range(1, members):
        pos_copy(d, me).start()

    def send_all(order):
        def act():
            for at in walk(order, sizes):
                for e in range(pair):
                    j = others.index((at["r"], at["c"], e))
                    if at["k"] == 0 and at["h"] == 0 and j:
                        kv_copy(j, mine).start()
                    if at["k"] == 1 and (at["h"] or j):
                        qg_copy(j, at["h"]).start()

        return act

    by_row(send_all(SEND_OUTER), send_all(SEND_INNER))

    dk_acc[...] = jnp.zeros_like(dk_acc)
    dv_acc[...] = jnp.zeros_like(dv_acc)
    pos_buf[me] = pos_mine[...]
    settled(pos_buf.at[pl.ds(0, members - 1)], pos_recv)
    settled(pos_buf.at[pl.ds(0, members - 1)], pos_send)

    def spread(i, carry):
        row = jnp.broadcast_to(
            pos_buf[mates * heads + i].astype(jnp.float32), (HEAD_DIM, width)
        )
        key_pos[i] = row.T[:rows]
        return carry

    lax.fori_loop(0, heads, spread, 0)
    settled(kv_buf.at[pl.ds(0, heads - 1)], kv_recv)

    def turn(s, carry):
        held = kv_buf[pl.ds(s * step, step), 0].reshape(step * rows, HEAD_DIM)
        key_t[s] = held.astype(jnp.float32).T.astype(jnp.bfloat16)
        return carry

    lax.fori_loop(0, steps, turn, 0)

    def pick(table, k):
        value = jnp.int32(table[0])
        for i, entry in enumerate(table[1:]):
            value = jnp.where(k == i + 1, entry, value)
        return value

    def tables_of(orders):
        tables = []
        for order in orders:
            table = [(at["h"], at["r"], at["c"]) for at in walk(order.strip("."), sizes)]
            if order.startswith("."):
                table.insert(0, table.pop(table.index((0, 0, 0))))
            tables.append(table)
        return tables

    stats_tables = tables_of((STATS_OUTER, STATS_INNER))
    grads_tables = tables_of((GRADS_OUTER, GRADS_INNER))
    lag = max(
        [LAG]
        + [
            there.index(((h - d) % ratio, r, c)) - k
            for table in grads_tables
            for k, (h, r, c) in enumerate(table)
            for there in stats_tables
            for d in range(ratio)
        ]
    )
    lag = min(lag, units)

    def unit_of(k, tables):
        tables = [[(h * lines + r) * across + c for h, r, c in table] for table in tables]
        n = jnp.where(outer, pick(tables[0], k), pick(tables[1], k))
        there = place_of(lax.rem(n // across, lines), lax.rem(n, across))
        return n, lax.rem(mates + n // wide, ratio) * wide + there

    def operand(unit, a):
        return qg_buf[pl.ds(unit * pair, pair), a].reshape(block, HEAD_DIM)

    def tiles(values):
        return values.reshape(step * rows // 8, 8, block)

    def stat_copy(unit, d, origin):
        return remote(
            stat_buf.at[mates, unit], stat_buf.at[origin, unit],
            stat_send, stat_recv.at[origin, unit],
            lax.rem(mates + d, ratio) * heads + mine, group,
        )

    def stats(k, carried):
        n, unit = unit_of(k, stats_tables)
        for c in range(pair):
            origin = unit * pair + c

            @pl.when(origin != me)
            def _():
                remote(
                    qg_buf.at[origin], qg_buf.at[origin], qg_send, qg_recv.at[origin],
                    me, group,
                ).wait_recv()

        query, grad = operand(unit, 0), operand(unit, 1)
        rows_of = [pos_buf[unit * pair + c].astype(jnp.float32)[:, :rows] for c in range(pair)]
        pos_row = jnp.concatenate(rows_of, axis=1) if pair > 1 else rows_of[0]

        def one(s, carry):
            top, total, delta = carry
            held = pl.ds(s * step, step)
            key = kv_buf[held, 0].reshape(step * rows, HEAD_DIM)
            value = kv_buf[held, 1].reshape(step * rows, HEAD_DIM)
            scores = lax.dot_general(key, query, NT, preferred_element_type=jnp.float32)
            key_held = key_pos[held].reshape(step * rows, HEAD_DIM)
            key_held = jnp.concatenate([key_held] * (block // HEAD_DIM), axis=1)
            scores = jnp.where(key_held <= pos_row, scores, LOW)
            here = jnp.max(jnp.max(tiles(scores), axis=0), axis=0, keepdims=True)
            new_top = jnp.maximum(top, here)
            unscaled = jnp.exp2((scores - new_top) * sharp)
            probs = lax.dot_general(value, grad, NT, preferred_element_type=jnp.float32)
            z_buf[n, s] = unscaled
            p_buf[n, s] = probs
            tops[n, s] = jnp.broadcast_to(new_top, (8, block))
            alpha = jnp.exp2((top - new_top) * sharp)
            total = total * alpha + jnp.sum(tiles(unscaled), axis=0)
            delta = delta * alpha + jnp.sum(tiles(unscaled * probs), axis=0)
            return new_top, total, delta

        zero = jnp.zeros((8, block), jnp.float32)
        top, total, delta = lax.fori_loop(
            0, steps, one, (jnp.full((1, block), LOW, jnp.float32), zero, zero)
        )
        total = jnp.sum(total, axis=0, keepdims=True)
        delta = jnp.sum(delta, axis=0, keepdims=True)
        stat_buf[mates, unit] = jnp.concatenate(
            [top, total, delta, jnp.zeros((5, block), jnp.float32)], axis=0
        )
        for d in range(1, ratio):
            stat_copy(unit, d, mates).start()
        return carried

    lax.fori_loop(0, lag, stats, 0)

    def grads(k, carried):
        n, unit = unit_of(k, grads_tables)
        for d in range(1, ratio):
            stat_copy(unit, d, lax.rem(mates + ratio - d, ratio)).wait_recv()
        whole = [stat_buf[d, unit] for d in range(ratio)]
        top = functools.reduce(jnp.maximum, [w[0:1] for w in whole])
        shares = [jnp.exp2((w[0:1] - top) * sharp) for w in whole]
        inverse = 1.0 / functools.reduce(jnp.add, [w[1:2] * s for w, s in zip(whole, shares)])
        delta = functools.reduce(jnp.add, [w[2:3] * s for w, s in zip(whole, shares)]) * inverse
        query, grad = operand(unit, 0), operand(unit, 1)

        def one(s, query_t):
            held = pl.ds(s * step, step)
            factor = jnp.exp2((tops[n, s][0:1] - top) * sharp) * inverse
            weights = z_buf[n, s] * factor
            grad_scores = (weights * (p_buf[n, s] - delta)).astype(jnp.bfloat16)
            value_term = jnp.dot(
                weights.astype(jnp.bfloat16), grad, preferred_element_type=jnp.float32
            )
            key_term = jnp.dot(grad_scores, query, preferred_element_type=jnp.float32)
            dv_acc[held] += value_term.reshape(step, rows, HEAD_DIM)
            dk_acc[held] += key_term.reshape(step, rows, HEAD_DIM)
            return query_t + jnp.dot(
                key_t[s], grad_scores, preferred_element_type=jnp.float32
            )

        query_t = lax.fori_loop(0, steps, one, jnp.zeros((HEAD_DIM, block), jnp.float32))
        grad_query = (query_t * scaling).T.astype(jnp.bfloat16)
        grad_query = grad_query.reshape(pair, groups, part_rows, HEAD_DIM)
        dq_stage[unit] = grad_query
        for c in range(pair):
            for e in range(groups):
                owner = unit * pair + c
                other = lax.rem(group + e, groups)
                copy = remote(
                    dq_stage.at[unit, c, other], dq_back.at[slot],
                    dq_send, dq_recv,
                    owner, other,
                )
                if e:
                    copy.start()
                else:
                    pl.when(owner != me)(copy.start)
        return carried

    def both(k, carried):
        stats(k, 0)
        grads(k - lag, 0)
        return carried

    if lag < units:
        lax.fori_loop(lag, units, both, 0)
    lax.fori_loop(units - lag, units, grads, 0)

    dq_back[slot] = dq_stage[me // pair, core, group]

    def back_copies(j, origin):
        return [
            remote(
                kv_final.at[j, a], out.at[:, columns(origin)], back_send,
                back_recv, mates * heads + ahead(j), group,
            )
            for a, out in enumerate((dk_out, dv_out))
        ]

    def finish(j):
        kv_final[j, 0] = (dk_acc[ahead(j)] * scaling).astype(jnp.bfloat16)
        kv_final[j, 1] = dv_acc[ahead(j)].astype(jnp.bfloat16)

    def give_back(order):
        def act():
            for at in walk(order, sizes):
                for e in range(pair):
                    j = others.index((at["r"], at["c"], e))
                    if j:
                        finish(j)
                        for copy in back_copies(j, mine):
                            copy.start()

        return act

    by_row(give_back(BACK_OUTER), give_back(BACK_INNER))
    finish(0)
    back_locals = [
        pltpu.make_async_copy(kv_final.at[0, a], out.at[:, columns(mine)], back_own.at[a])
        for a, out in enumerate((dk_out, dv_out))
    ]
    for copy in back_locals:
        copy.start()

    settled(qg_buf.at[pl.ds(0, members - 1)], qg_send)
    settled(kv_buf.at[pl.ds(0, heads - 1)], kv_send)
    settled(stat_buf.at[pl.ds(0, ratio - 1)], stat_send)
    settled(dq_back.at[pl.ds(0, members * groups - 1)], dq_recv)
    for h in range(groups * heads):
        parts = [
            dq_back[d * groups * heads + h].astype(jnp.float32) for d in range(ratio)
        ]
        dq_sum[:, h * HEAD_DIM:(h + 1) * HEAD_DIM] = functools.reduce(jnp.add, parts).astype(
            jnp.bfloat16
        )
    dq_local = pltpu.make_async_copy(dq_sum, dq_out, dq_own)
    dq_local.start()
    settled(dq_back.at[pl.ds(0, members * groups - 1)], dq_send)
    settled(kv_final.at[pl.ds(0, heads - 1)], back_send)
    settled(kv_final.at[pl.ds(0, heads - 1)], back_recv)
    for copy in back_locals + [dq_local]:
        copy.wait()


def settle(a_in, b_in, c_in, a_out, b_out, c_out, a_mid, b_mid, c_mid, come, go):
    ins = [
        pltpu.make_async_copy(source, middle, come.at[i])
        for i, (source, middle) in enumerate(((a_in, a_mid), (b_in, b_mid), (c_in, c_mid)))
    ]
    outs = [
        pltpu.make_async_copy(middle, sink, go.at[i])
        for i, (middle, sink) in enumerate(((a_mid, a_out), (b_mid, b_out), (c_mid, c_out)))
    ]
    for copy in ins:
        copy.start()
    for copy, then in zip(ins, outs):
        copy.wait()
        then.start()
    for copy in outs:
        copy.wait()


def local(members, groups, query_rows, key_rows, value_rows, grad_output, positions):
    rows, wide = query_rows.shape
    heads = wide // HEAD_DIM
    ratio = members // heads
    width = -(-rows // HEAD_DIM) * HEAD_DIM
    pair = math.gcd(heads, PAIR)
    step = math.gcd(heads, STEP)
    units = members // pair
    block = pair * rows
    position_rows = positions[None]
    low, full = jnp.bfloat16, jnp.float32
    piece = (rows, HEAD_DIM)
    dma = pltpu.SemaphoreType.DMA
    scratch = [
        pltpu.VMEM((members, 2) + piece, low),
        pltpu.VMEM((heads, 2) + piece, low),
        pltpu.VMEM((heads, 2) + piece, low),
        pltpu.VMEM((heads, 2) + piece, low),
        pltpu.VMEM((heads // step, HEAD_DIM, step * rows), low),
        pltpu.VMEM((1, width), jnp.int32),
        pltpu.VMEM((members, 1, width), jnp.int32),
        pltpu.VMEM((heads,) + piece, full),
        pltpu.VMEM((units, heads // step, 8, block), full),
        pltpu.VMEM((units, heads // step, step * rows, block), full),
        pltpu.VMEM((units, heads // step, step * rows, block), full),
        pltpu.VMEM((heads,) + piece, full),
        pltpu.VMEM((heads,) + piece, full),
        pltpu.VMEM((ratio, units, 8, block), full),
        pltpu.VMEM((heads, 2) + piece, low),
        pltpu.VMEM((units, pair, groups, rows // groups, HEAD_DIM), low),
        pltpu.VMEM((members * groups, rows // groups, HEAD_DIM), low),
        pltpu.VMEM((rows // groups, groups * wide), low),
        dma, dma, dma, dma((members,)), dma, dma, dma, dma,
        dma, dma((ratio, units)), dma, dma, dma((2,)), dma, dma, dma,
    ]
    vmem = pl.BlockSpec(memory_space=pltpu.VMEM)
    hbm = pl.BlockSpec(memory_space=pl.ANY)
    results = pl.pallas_call(
        functools.partial(kernel, members, heads, groups, rows, width, pair, step),
        out_shape=(
            jax.ShapeDtypeStruct((rows // groups, groups * wide), low),
            jax.ShapeDtypeStruct((rows, wide), low),
            jax.ShapeDtypeStruct((rows, wide), low),
        ),
        in_specs=[vmem, hbm, hbm, hbm, hbm],
        out_specs=(hbm, hbm, hbm),
        scratch_shapes=scratch,
        compiler_params=pltpu.CompilerParams(
            collective_id=0, has_side_effects=True, vmem_limit_bytes=63 * 1024 * 1024
        ),
    )(position_rows, query_rows, key_rows, value_rows, grad_output)
    return pl.pallas_call(
        settle,
        out_shape=tuple(jax.ShapeDtypeStruct(r.shape, r.dtype) for r in results),
        in_specs=[hbm, hbm, hbm],
        out_specs=(hbm, hbm, hbm),
        scratch_shapes=[pltpu.VMEM(r.shape, r.dtype) for r in results] + [dma((3,)), dma((3,))],
    )(*results)


def solution(mesh):
    placed = (P("seq", "head"), P("seq", "head"), P("seq", "head"), P("seq", "head"), P("seq"))
    return jax.shard_map(
        functools.partial(local, mesh.shape["seq"], mesh.shape["head"]),
        mesh=mesh,
        in_specs=placed,
        out_specs=(P(("seq", "head"), None), P("seq", "head"), P("seq", "head")),
        check_vma=False,
    )
```

```python
import functools
import math

import jax
import jax.numpy as jnp
from jax import lax
from jax.experimental import pallas as pl
from jax.experimental.pallas import tpu as pltpu
from jax.sharding import PartitionSpec as P

HEAD_DIM = 128
MESH = pl.DeviceIdType.MESH
NT = (((1,), (1,)), ((), ()))
LOW = -1e30
LAG = 6
PAIR = 2
STEP = 8
SEND_OUTER, SEND_INNER = "kCRh", "kCRh"
STATS_OUTER, STATS_INNER = ".CRh", ".CRh"
GRADS_OUTER, GRADS_INNER = "CRH", "CRH"
BACK_OUTER, BACK_INNER = "RC", "RC"


def walk(order, sizes):
    found = [{}]
    for axis in order:
        values = list(range(sizes[axis.lower()]))
        if axis.isupper():
            values.reverse()
        found = [{**one, axis.lower(): v} for one in found for v in values]
    return found


def kernel(
    members, heads, groups, rows, width, pair, step,
    pos_ref, q_hbm, k_hbm, v_hbm, g_hbm,
    dq_out, dk_out, dv_out,
    qg_buf, kv_buf, qg_stage, kv_stage, key_t, pos_mine, pos_buf, key_pos, tops,
    z_buf, p_buf, dk_acc, dv_acc, stat_buf, kv_final, dq_stage, dq_back, dq_sum,
    qg_local, kv_local, qg_send, qg_recv, kv_send, kv_recv, pos_send, pos_recv,
    stat_send, stat_recv, back_send, back_recv, back_own, dq_send, dq_recv, dq_own,
):
    ratio = members // heads
    units = members // pair
    wide = heads // pair
    lines = 2 if wide % 2 == 0 else 1
    across = wide // lines
    sizes = {"h": ratio, "r": lines, "c": across, "k": 2}
    me = lax.axis_index("seq")
    group = lax.axis_index("head")
    mine = lax.rem(me, heads)
    mates = me // heads
    place = mine // pair
    core = lax.rem(mine, pair)
    line = place // across
    column = lax.rem(place, across)
    outer = (2 * mates < ratio) == (2 * line < lines)
    scaling = HEAD_DIM ** (-0.5)
    sharp = scaling / math.log(2.0)
    slot = (mates * groups + group) * heads + mine
    block = pair * rows
    steps = heads // step
    part_rows = rows // groups

    barrier = pltpu.get_barrier_semaphore()
    for d in range(members):
        for e in range(groups):
            if d or e:
                pl.semaphore_signal(
                    barrier, inc=1,
                    device_id={
                        "seq": lax.rem(me + d, members), "head": lax.rem(group + e, groups),
                    },
                    device_id_type=MESH,
                )

    def by_row(act_outer, act_inner):
        pl.when(outer)(act_outer)
        pl.when(jnp.logical_not(outer))(act_inner)

    def columns(index):
        return pl.ds(pl.multiple_of(index * HEAD_DIM, HEAD_DIM), HEAD_DIM)

    others = [(r, c, e) for r in range(lines) for c in range(across) for e in range(pair)]

    def place_of(r, c):
        return lax.rem(line + r, lines) * across + lax.rem(column + c, across)

    def ahead(j):
        r, c, e = others[j]
        return place_of(r, c) * pair + lax.rem(core + e, pair)

    def behind(j):
        r, c, e = others[j]
        return place_of(lines - r, across - c) * pair + lax.rem(core + pair - e, pair)

    def local_copies(arrays, first, stage, sems, j):
        return [
            pltpu.make_async_copy(
                array.at[:, columns(ahead(j))], first.at[a] if j == 0 else stage.at[j, a],
                sems,
            )
            for a, array in enumerate(arrays)
        ]

    kv_locals = [
        local_copies((k_hbm, v_hbm), kv_buf.at[mine], kv_stage, kv_local, j)
        for j in range(heads)
    ]
    qg_locals = [
        local_copies((q_hbm, g_hbm), qg_buf.at[me], qg_stage, qg_local, j) for j in range(heads)
    ]
    for copies in kv_locals + qg_locals:
        for copy in copies:
            copy.start()

    pos_mine[...] = jnp.zeros_like(pos_mine)
    pos_mine[:, :rows] = pos_ref[...]
    pl.semaphore_wait(barrier, members * groups - 1)

    def remote(source, sink, send, recv, seq, head):
        return pltpu.make_async_remote_copy(
            src_ref=source, dst_ref=sink, send_sem=send, recv_sem=recv,
            device_id={"seq": seq, "head": head}, device_id_type=MESH,
        )

    def pos_copy(d, origin):
        return remote(
            pos_mine, pos_buf.at[origin], pos_send, pos_recv,
            lax.rem(me + d, members), group,
        )

    def kv_copy(j, origin):
        return remote(
            kv_stage.at[j], kv_buf.at[origin], kv_send, kv_recv,
            mates * heads + ahead(j), group,
        )

    def qg_copy(j, d):
        source = qg_buf.at[me] if j == 0 else qg_stage.at[j]
        return remote(
            source, qg_buf.at[me], qg_send, qg_recv.at[me],
            lax.rem(mates + d, ratio) * heads + ahead(j), group,
        )

    def settled(ref, sem):
        remote(ref, ref, sem, sem, me, group).wait_recv()

    settled(kv_stage, kv_local)
    settled(qg_stage, qg_local)
    for d in range(1, members):
        pos_copy(d, me).start()

    def send_all(order):
        def act():
            for at in walk(order, sizes):
                for e in range(pair):
                    j = others.index((at["r"], at["c"], e))
                    if at["k"] == 0 and at["h"] == 0 and j:
                        kv_copy(j, mine).start()
                    if at["k"] == 1 and (at["h"] or j):
                        qg_copy(j, at["h"]).start()

        return act

    by_row(send_all(SEND_OUTER), send_all(SEND_INNER))

    dk_acc[...] = jnp.zeros_like(dk_acc)
    dv_acc[...] = jnp.zeros_like(dv_acc)
    pos_buf[me] = pos_mine[...]
    settled(pos_buf.at[pl.ds(0, members - 1)], pos_recv)
    settled(pos_buf.at[pl.ds(0, members - 1)], pos_send)

    def spread(i, carry):
        row = jnp.broadcast_to(
            pos_buf[mates * heads + i].astype(jnp.float32), (HEAD_DIM, width)
        )
        key_pos[i] = row.T[:rows]
        return carry

    lax.fori_loop(0, heads, spread, 0)
    settled(kv_buf.at[pl.ds(0, heads - 1)], kv_recv)

    def turn(s, carry):
        held = kv_buf[pl.ds(s * step, step), 0].reshape(step * rows, HEAD_DIM)
        key_t[s] = held.astype(jnp.float32).T.astype(jnp.bfloat16)
        return carry

    lax.fori_loop(0, steps, turn, 0)

    def pick(table, k):
        value = jnp.int32(table[0])
        for i, entry in enumerate(table[1:]):
            value = jnp.where(k == i + 1, entry, value)
        return value

    def tables_of(orders):
        tables = []
        for order in orders:
            table = [(at["h"], at["r"], at["c"]) for at in walk(order.strip("."), sizes)]
            if order.startswith("."):
                table.insert(0, table.pop(table.index((0, 0, 0))))
            tables.append(table)
        return tables

    stats_tables = tables_of((STATS_OUTER, STATS_INNER))
    grads_tables = tables_of((GRADS_OUTER, GRADS_INNER))
    lag = max(
        [LAG]
        + [
            there.index(((h - d) % ratio, r, c)) - k
            for table in grads_tables
            for k, (h, r, c) in enumerate(table)
            for there in stats_tables
            for d in range(ratio)
        ]
    )
    lag = min(lag, units)

    def unit_of(k, tables):
        tables = [[(h * lines + r) * across + c for h, r, c in table] for table in tables]
        n = jnp.where(outer, pick(tables[0], k), pick(tables[1], k))
        there = place_of(lax.rem(n // across, lines), lax.rem(n, across))
        return n, lax.rem(mates + n // wide, ratio) * wide + there

    def operand(unit, a):
        return qg_buf[pl.ds(unit * pair, pair), a].reshape(block, HEAD_DIM)

    def tiles(values):
        return values.reshape(step * rows // 8, 8, block)

    def stat_copy(unit, d, origin):
        return remote(
            stat_buf.at[mates, unit], stat_buf.at[origin, unit],
            stat_send, stat_recv.at[origin, unit],
            lax.rem(mates + d, ratio) * heads + mine, group,
        )

    def stats(k, carried):
        n, unit = unit_of(k, stats_tables)
        for c in range(pair):
            origin = unit * pair + c

            @pl.when(origin != me)
            def _():
                remote(
                    qg_buf.at[origin], qg_buf.at[origin], qg_send, qg_recv.at[origin],
                    me, group,
                ).wait_recv()

        query, grad = operand(unit, 0), operand(unit, 1)
        rows_of = [pos_buf[unit * pair + c].astype(jnp.float32)[:, :rows] for c in range(pair)]
        pos_row = jnp.concatenate(rows_of, axis=1) if pair > 1 else rows_of[0]

        def one(s, carry):
            top, total, delta = carry
            held = pl.ds(s * step, step)
            key = kv_buf[held, 0].reshape(step * rows, HEAD_DIM)
            value = kv_buf[held, 1].reshape(step * rows, HEAD_DIM)
            scores = lax.dot_general(key, query, NT, preferred_element_type=jnp.float32)
            key_held = key_pos[held].reshape(step * rows, HEAD_DIM)
            key_held = jnp.concatenate([key_held] * (block // HEAD_DIM), axis=1)
            scores = jnp.where(key_held <= pos_row, scores, LOW)
            here = jnp.max(jnp.max(tiles(scores), axis=0), axis=0, keepdims=True)
            new_top = jnp.maximum(top, here)
            unscaled = jnp.exp2((scores - new_top) * sharp)
            probs = lax.dot_general(value, grad, NT, preferred_element_type=jnp.float32)
            z_buf[n, s] = unscaled
            p_buf[n, s] = probs
            tops[n, s] = jnp.broadcast_to(new_top, (8, block))
            alpha = jnp.exp2((top - new_top) * sharp)
            total = total * alpha + jnp.sum(tiles(unscaled), axis=0)
            delta = delta * alpha + jnp.sum(tiles(unscaled * probs), axis=0)
            return new_top, total, delta

        zero = jnp.zeros((8, block), jnp.float32)
        top, total, delta = lax.fori_loop(
            0, steps, one, (jnp.full((1, block), LOW, jnp.float32), zero, zero)
        )
        total = jnp.sum(total, axis=0, keepdims=True)
        delta = jnp.sum(delta, axis=0, keepdims=True)
        stat_buf[mates, unit] = jnp.concatenate(
            [top, total, delta, jnp.zeros((5, block), jnp.float32)], axis=0
        )
        for d in range(1, ratio):
            stat_copy(unit, d, mates).start()
        return carried

    lax.fori_loop(0, lag, stats, 0)

    def grads(k, carried):
        n, unit = unit_of(k, grads_tables)
        for d in range(1, ratio):
            stat_copy(unit, d, lax.rem(mates + ratio - d, ratio)).wait_recv()
        whole = [stat_buf[d, unit] for d in range(ratio)]
        top = functools.reduce(jnp.maximum, [w[0:1] for w in whole])
        shares = [jnp.exp2((w[0:1] - top) * sharp) for w in whole]
        inverse = 1.0 / functools.reduce(jnp.add, [w[1:2] * s for w, s in zip(whole, shares)])
        delta = functools.reduce(jnp.add, [w[2:3] * s for w, s in zip(whole, shares)]) * inverse
        query, grad = operand(unit, 0), operand(unit, 1)

        def one(s, query_t):
            held = pl.ds(s * step, step)
            factor = jnp.exp2((tops[n, s][0:1] - top) * sharp) * inverse
            weights = z_buf[n, s] * factor
            grad_scores = (weights * (p_buf[n, s] - delta)).astype(jnp.bfloat16)
            value_term = jnp.dot(
                weights.astype(jnp.bfloat16), grad, preferred_element_type=jnp.float32
            )
            key_term = jnp.dot(grad_scores, query, preferred_element_type=jnp.float32)
            dv_acc[held] += value_term.reshape(step, rows, HEAD_DIM)
            dk_acc[held] += key_term.reshape(step, rows, HEAD_DIM)
            return query_t + jnp.dot(
                key_t[s], grad_scores, preferred_element_type=jnp.float32
            )

        query_t = lax.fori_loop(0, steps, one, jnp.zeros((HEAD_DIM, block), jnp.float32))
        grad_query = (query_t * scaling).T.astype(jnp.bfloat16)
        grad_query = grad_query.reshape(pair, groups, part_rows, HEAD_DIM)
        dq_stage[unit] = grad_query
        for c in range(pair):
            for e in range(groups):
                owner = unit * pair + c
                other = lax.rem(group + e, groups)
                copy = remote(
                    dq_stage.at[unit, c, other], dq_back.at[slot],
                    dq_send, dq_recv,
                    owner, other,
                )
                if e:
                    copy.start()
                else:
                    pl.when(owner != me)(copy.start)
        return carried

    def both(k, carried):
        stats(k, 0)
        grads(k - lag, 0)
        return carried

    if lag < units:
        lax.fori_loop(lag, units, both, 0)
    lax.fori_loop(units - lag, units, grads, 0)

    dq_back[slot] = dq_stage[me // pair, core, group]

    def back_copies(j, origin):
        return [
            remote(
                kv_final.at[j, a], out.at[:, columns(origin)], back_send,
                back_recv, mates * heads + ahead(j), group,
            )
            for a, out in enumerate((dk_out, dv_out))
        ]

    def finish(j):
        kv_final[j, 0] = (dk_acc[ahead(j)] * scaling).astype(jnp.bfloat16)
        kv_final[j, 1] = dv_acc[ahead(j)].astype(jnp.bfloat16)

    def give_back(order):
        def act():
            for at in walk(order, sizes):
                for e in range(pair):
                    j = others.index((at["r"], at["c"], e))
                    if j:
                        finish(j)
                        for copy in back_copies(j, mine):
                            copy.start()

        return act

    by_row(give_back(BACK_OUTER), give_back(BACK_INNER))
    finish(0)
    back_locals = [
        pltpu.make_async_copy(kv_final.at[0, a], out.at[:, columns(mine)], back_own.at[a])
        for a, out in enumerate((dk_out, dv_out))
    ]
    for copy in back_locals:
        copy.start()

    settled(qg_buf.at[pl.ds(0, members - 1)], qg_send)
    settled(kv_buf.at[pl.ds(0, heads - 1)], kv_send)
    settled(stat_buf.at[pl.ds(0, ratio - 1)], stat_send)
    settled(dq_back.at[pl.ds(0, members * groups - 1)], dq_recv)
    for h in range(groups * heads):
        parts = [
            dq_back[d * groups * heads + h].astype(jnp.float32) for d in range(ratio)
        ]
        dq_sum[:, h * HEAD_DIM:(h + 1) * HEAD_DIM] = functools.reduce(jnp.add, parts).astype(
            jnp.bfloat16
        )
    dq_local = pltpu.make_async_copy(dq_sum, dq_out, dq_own)
    dq_local.start()
    settled(dq_back.at[pl.ds(0, members * groups - 1)], dq_send)
    settled(kv_final.at[pl.ds(0, heads - 1)], back_send)
    settled(kv_final.at[pl.ds(0, heads - 1)], back_recv)
    for copy in back_locals + [dq_local]:
        copy.wait()


def settle(a_in, b_in, c_in, a_out, b_out, c_out, a_mid, b_mid, c_mid, come, go):
    ins = [
        pltpu.make_async_copy(source, middle, come.at[i])
        for i, (source, middle) in enumerate(((a_in, a_mid), (b_in, b_mid), (c_in, c_mid)))
    ]
    outs = [
        pltpu.make_async_copy(middle, sink, go.at[i])
        for i, (middle, sink) in enumerate(((a_mid, a_out), (b_mid, b_out), (c_mid, c_out)))
    ]
    for copy in ins:
        copy.start()
    for copy, then in zip(ins, outs):
        copy.wait()
        then.start()
    for copy in outs:
        copy.wait()


def local(members, groups, query_rows, key_rows, value_rows, grad_output, positions):
    rows, wide = query_rows.shape
    heads = wide // HEAD_DIM
    ratio = members // heads
    width = -(-rows // HEAD_DIM) * HEAD_DIM
    pair = math.gcd(heads, PAIR)
    step = math.gcd(heads, STEP)
    units = members // pair
    block = pair * rows
    position_rows = positions[None]
    low, full = jnp.bfloat16, jnp.float32
    piece = (rows, HEAD_DIM)
    dma = pltpu.SemaphoreType.DMA
    scratch = [
        pltpu.VMEM((members, 2) + piece, low),
        pltpu.VMEM((heads, 2) + piece, low),
        pltpu.VMEM((heads, 2) + piece, low),
        pltpu.VMEM((heads, 2) + piece, low),
        pltpu.VMEM((heads // step, HEAD_DIM, step * rows), low),
        pltpu.VMEM((1, width), jnp.int32),
        pltpu.VMEM((members, 1, width), jnp.int32),
        pltpu.VMEM((heads,) + piece, full),
        pltpu.VMEM((units, heads // step, 8, block), full),
        pltpu.VMEM((units, heads // step, step * rows, block), full),
        pltpu.VMEM((units, heads // step, step * rows, block), full),
        pltpu.VMEM((heads,) + piece, full),
        pltpu.VMEM((heads,) + piece, full),
        pltpu.VMEM((ratio, units, 8, block), full),
        pltpu.VMEM((heads, 2) + piece, low),
        pltpu.VMEM((units, pair, groups, rows // groups, HEAD_DIM), low),
        pltpu.VMEM((members * groups, rows // groups, HEAD_DIM), low),
        pltpu.VMEM((rows // groups, groups * wide), low),
        dma, dma, dma, dma((members,)), dma, dma, dma, dma,
        dma, dma((ratio, units)), dma, dma, dma((2,)), dma, dma, dma,
    ]
    vmem = pl.BlockSpec(memory_space=pltpu.VMEM)
    hbm = pl.BlockSpec(memory_space=pl.ANY)
    results = pl.pallas_call(
        functools.partial(kernel, members, heads, groups, rows, width, pair, step),
        out_shape=(
            jax.ShapeDtypeStruct((rows // groups, groups * wide), low),
            jax.ShapeDtypeStruct((rows, wide), low),
            jax.ShapeDtypeStruct((rows, wide), low),
        ),
        in_specs=[vmem, hbm, hbm, hbm, hbm],
        out_specs=(hbm, hbm, hbm),
        scratch_shapes=scratch,
        compiler_params=pltpu.CompilerParams(
            collective_id=0, has_side_effects=True, vmem_limit_bytes=63 * 1024 * 1024
        ),
    )(position_rows, query_rows, key_rows, value_rows, grad_output)
    return pl.pallas_call(
        settle,
        out_shape=tuple(jax.ShapeDtypeStruct(r.shape, r.dtype) for r in results),
        in_specs=[hbm, hbm, hbm],
        out_specs=(hbm, hbm, hbm),
        scratch_shapes=[pltpu.VMEM(r.shape, r.dtype) for r in results] + [dma((3,)), dma((3,))],
    )(*results)


def solution(mesh):
    placed = (P("seq", "head"), P("seq", "head"), P("seq", "head"), P("seq", "head"), P("seq"))
    return jax.shard_map(
        functools.partial(local, mesh.shape["seq"], mesh.shape["head"]),
        mesh=mesh,
        in_specs=placed,
        out_specs=(P(("seq", "head"), None), P("seq", "head"), P("seq", "head")),
        check_vma=False,
    )
```
